32 devices in a mesh: tm: 32 (over z, y, x, core), prod: 1.
Axes of the slice: x: 2, y: 2, z: 4, core: 2. Of those that a mesh axis runs over, the one named last changes fastest.
Arguments:
- sales_records: float32 [1024, 16, 16, 128], P('tm', 'prod'), may hold values from -6 to 6
- day_month: int32 [1024], replicated, may hold values from 0 to 31, as said below
- month_year: int32 [32], replicated, may hold values from 0 to 3, never falling along the last dimension, each value on 1 to 16 neighbouring positions
- product_category: int32 [16], replicated, may hold values from 0 to 31
- store_region: int32 [16], replicated, may hold values from 0 to 3
Outputs:
- month_detail: float32 [32, 32, 4, 128], P('tm', 'prod')
- month_category: float32 [32, 32, 128], P('tm', 'prod')
- month_region: float32 [32, 4, 128], P('tm')
- month_totals: float32 [32, 128], P('tm')
- year_detail: float32 [4, 32, 4, 128], replicated
- year_category: float32 [4, 32, 128], replicated
- year_region: float32 [4, 4, 128], replicated
- year_totals: float32 [4, 128], replicated
The draws below stay inside these ranges and needn't reach their ends.
Inputs may be any that keep to these rules, and one draw needn't show every extreme that they name: `day_month`: never falls along the days; month m, for m of 1 to 31, begins at a day from m * 32 - 31 // 2 to m * 32 + 31 // 2, and both ends of that range are taken in every draw. `month_year`: never falls along the months; every year has 1 to 16 months, one exactly that many.
All inputs are finite; a program needn't handle non-finite values.
Results may differ from the reference program's by a relative error of at most 0.0001.
Values sent between devices are 32-bit elements; how exact they have to be, the bound alone decides.
No kernel may reach another device: no remote copies, remote signals or barrier semaphores. Data moves between devices by JAX's collectives and lax.ppermute only.
A program may use at most 64 MiB of HBM per device.

```python
import math
import jax
import jax.numpy as jnp
import numpy as np
from jax import lax

DAYS_PER_INDEX = 32
STORE_COUNT = 16
MEASURE_COUNT = 128
CATEGORY_COUNT = 32
REGION_COUNT = 4
TOTAL_DAYS = 1024
PRODUCT_COUNT = 16
TOTAL_MONTHS = 32
YEARS = 4
N_TM = 32


def draw_day_month(key, part):
    half = (DAYS_PER_INDEX - 1) // 2
    inner = TOTAL_MONTHS - 1
    jitter = jax.random.randint(jax.random.fold_in(key, 11), (inner,), -half, half + 1)
    places = jnp.arange(inner, dtype=jnp.int32)
    middle = TOTAL_MONTHS // 2
    jitter = jnp.where(places == 0, -half, jitter)
    jitter = jnp.where(places == middle - 2, -half, jitter)
    jitter = jnp.where(places == middle - 1, half, jitter)
    jitter = jnp.where(places == middle, half, jitter)
    bounds = (places + 1) * DAYS_PER_INDEX + jitter
    days = jnp.arange(TOTAL_DAYS, dtype=jnp.int32)
    return jnp.sum((days[:, None] >= bounds[None, :]).astype(jnp.int32), 1).astype(jnp.int32)


def with_ends(result, rng, low, high):
    dims = result.shape
    place = [jax.random.randint(jax.random.fold_in(rng, axis), (), 0, dims[axis]) for axis in range(len(dims))]
    result = result.at[tuple(place)].set(low)
    longest = dims.index(max(dims))
    place[longest] = (place[longest] + 1) % dims[longest]
    return result.at[tuple(place)].set(high)


def shard_levels(own_key, extent, split, smallest, top_value):
    def one(position, parts):
        draws = jax.random.uniform(jax.random.fold_in(jax.random.fold_in(own_key, 6), position), (parts,), jnp.float32, smallest / len(split), top_value / len(split))
        return jnp.repeat(jnp.exp(draws), extent[position] // parts).reshape((-1,) + (1,) * (len(extent) - position - 1))

    factor_of = one(*split[0])
    for cut in split[1:]:
        factor_of = factor_of * one(*cut)
    return factor_of


def length_profile(number_of, total, bound, slope):
    loads = [(1 << 20) // math.isqrt(grade ** slope) + 1 for grade in range(2, number_of + 1)]
    spare, given = total - bound - (number_of - 1), [1] * (number_of - 1)
    while spare > 0:
        movable = [i for i in range(number_of - 1) if given[i] < bound]
        pool, left = sum([loads[i] for i in movable]), spare
        for i in movable:
            addition = min(bound - given[i], max(1, left * loads[i] // pool), spare)
            given[i] = given[i] + addition
            spare = spare - addition
    return np.array([bound] + given)


def ragged_sizes(rng, amount, total, reach, slope):
    if amount == 2:
        one = jax.random.randint(rng, (), max(1, total - reach), min(reach, total - 1) + 1)
        return jnp.stack([one, total - one])
    sizes = jnp.asarray(length_profile(amount, total, reach, slope), jnp.int32)
    pairs = (amount - 1) // 2
    donor, sink = sizes[1:1 + 2 * pairs:2], sizes[2:2 + 2 * pairs:2]
    margin = jnp.minimum(donor - 1, reach - sink)
    passed = jax.random.randint(jax.random.fold_in(rng, 1), (pairs,), 0, 1 << 20) % (margin + 1)
    sizes = sizes.at[1:1 + 2 * pairs:2].set(donor - passed).at[2:2 + 2 * pairs:2].set(sink + passed)
    return sizes[jax.random.permutation(jax.random.fold_in(rng, 2), amount)]


def bell_draw(own_key, dims, deviation, limit, shards=(), held_as=jnp.bfloat16):
    entries = deviation * jax.random.normal(own_key, dims, jnp.float32)
    if shards:
        entries = entries * shard_levels(own_key, dims, shards, -0.22, 0.18)
    return jnp.clip(entries, -limit, limit).astype(held_as)


def setup_inputs(seed: int = 0) -> dict:
    keys = jax.random.split(jax.random.key(seed), 6)
    sales_records = bell_draw(keys[0], (TOTAL_DAYS, PRODUCT_COUNT, STORE_COUNT, MEASURE_COUNT), 1.0, 6.0, ((0, 32),), jnp.float32)
    day_month = draw_day_month(jax.random.fold_in(keys[5], 71), 0)
    month_year = jnp.searchsorted(jnp.cumsum(ragged_sizes(keys[2], YEARS, TOTAL_MONTHS, 2 * TOTAL_MONTHS // YEARS, 1)), jnp.arange(TOTAL_MONTHS), side="right").astype(jnp.int32)
    product_category = with_ends(jax.random.randint(keys[3], (PRODUCT_COUNT,), 0, CATEGORY_COUNT), jax.random.fold_in(keys[3], 1), 0, CATEGORY_COUNT - 1).astype(jnp.int32)
    store_region = with_ends(jax.random.randint(keys[4], (STORE_COUNT,), 0, REGION_COUNT), jax.random.fold_in(keys[4], 1), 0, REGION_COUNT - 1).astype(jnp.int32)
    return dict(sales_records=sales_records, day_month=day_month, month_year=month_year, product_category=product_category, store_region=store_region)


def onehot(labels, width):
    return (labels[:, None] == jnp.arange(width, dtype=jnp.int32)[None, :]).astype(jnp.float32)

def scaled(sums, counts):
    return sums / jnp.sqrt(counts)

def reference(sales_records, day_month, month_year, product_category, store_region):
    highest = lax.Precision.HIGHEST
    month_hot = onehot(day_month, TOTAL_MONTHS)
    year_hot = onehot(month_year, YEARS)
    category_hot = onehot(product_category, CATEGORY_COUNT)
    region_hot = onehot(store_region, REGION_COUNT)
    daily_blocks = sales_records.reshape(N_TM, DAYS_PER_INDEX, PRODUCT_COUNT, STORE_COUNT, MEASURE_COUNT)
    month_blocks = month_hot.reshape(N_TM, DAYS_PER_INDEX, TOTAL_MONTHS)

    def accumulate(running, pieces):
        day_block, block_hot = pieces
        by_region = jnp.einsum('dpsq,sr->dprq', day_block, region_hot, precision=highest)
        by_category = jnp.einsum('dprq,pc->dcrq', by_region, category_hot, precision=highest)
        return (running + jnp.einsum('dcrq,dm->mcrq', by_category, block_hot, precision=highest), None)
    start_offset = jnp.zeros((TOTAL_MONTHS, CATEGORY_COUNT, REGION_COUNT, MEASURE_COUNT), jnp.float32)
    cube, _ = lax.scan(accumulate, start_offset, (daily_blocks, month_blocks))
    year_cube = jnp.einsum('mcrq,my->ycrq', cube, year_hot, precision=highest)
    month_days = lax.optimization_barrier(jnp.sum(month_hot, 0))
    year_days = jnp.dot(month_days, year_hot, precision=highest)
    category_size = lax.optimization_barrier(jnp.sum(category_hot, 0))
    region_size = lax.optimization_barrier(jnp.sum(region_hot, 0))
    stores = float(STORE_COUNT)
    products = float(PRODUCT_COUNT)

    def four_nodes(detail, period_days):
        cell = period_days[:, None, None] * category_size[None, :, None] * region_size[None, None, :]
        first = scaled(detail, jnp.maximum(cell, 1.0)[..., None])
        by_cat = lax.optimization_barrier(jnp.sum(detail, 2))
        second = scaled(by_cat, jnp.maximum(period_days[:, None] * category_size[None, :] * stores, 1.0)[..., None])
        by_reg = lax.optimization_barrier(jnp.sum(detail, 1))
        third = scaled(by_reg, jnp.maximum(period_days[:, None] * products * region_size[None, :], 1.0)[..., None])
        fourth = scaled(lax.optimization_barrier(jnp.sum(by_reg, 1)), (period_days * products * stores)[:, None])
        return (first, second, third, fourth)
    month_detail, month_category, month_region, month_totals = four_nodes(cube, month_days)
    year_detail, year_category, year_region, year_totals = four_nodes(year_cube, year_days)
    return (month_detail, month_category, month_region, month_totals, year_detail, year_category, year_region, year_totals)
```

```python
import jax
import jax.numpy as jnp
from jax import lax
from jax.experimental import pallas as pl
from jax.experimental.pallas import tpu as pltpu
from jax.sharding import PartitionSpec as P

CATEGORY_COUNT = 32
REGION_COUNT = 4
CHUNKS = 8
VMEM = pl.BlockSpec(memory_space=pltpu.VMEM)
SMEM = pl.BlockSpec(memory_space=pltpu.SMEM)
ANY = pl.BlockSpec(memory_space=pl.ANY)


def log2(n):
    assert n & (n - 1) == 0
    return n.bit_length() - 1


def div(x, n):
    return lax.shift_right_logical(x, jnp.int32(log2(n)))


def mod(x, n):
    return lax.bitwise_and(x, jnp.int32(n - 1))


def pieces(x):
    high = x.astype(jnp.bfloat16)
    rest = x - high.astype(jnp.float32)
    mid = rest.astype(jnp.bfloat16)
    low = (rest - mid.astype(jnp.float32)).astype(jnp.bfloat16)
    return [high, mid, low]


def select_rows(hot, blocks):
    width = blocks[0].shape[1]
    out = jnp.dot(
        hot, jnp.concatenate([t for b in blocks for t in pieces(b)], axis=1), preferred_element_type=jnp.float32
    )
    cut = [out[:, i * width : (i + 1) * width] for i in range(3 * len(blocks))]
    return [(cut[3 * i + 2] + cut[3 * i + 1]) + cut[3 * i] for i in range(len(blocks))]


def local_sums(sales, day_month, month_year, store_region, year_count):
    days, products, stores, measures = sales.shape
    cells = products * REGION_COUNT
    half = year_count // 2
    step = days // CHUNKS
    months = month_year.shape[0]

    def kernel(sales_hbm, dm_hbm, my_hbm, sr_hbm, keep, send, own, far, buf, dm, my, sr, acc, sems, small):
        t = lax.axis_index("tm")
        b = lax.rem(t, 2)
        copies = [
            pltpu.make_async_copy(s, d, small.at[i])
            for i, (s, d) in enumerate(((dm_hbm, dm), (my_hbm, my), (sr_hbm, sr)))
        ]
        for c in copies:
            c.start()
        loads = [
            pltpu.make_async_copy(sales_hbm.at[pl.ds(i * step, step)], buf.at[pl.ds(i * step, step)], sems.at[i])
            for i in range(CHUNKS)
        ]
        for c in loads:
            c.start()
        for c in copies:
            c.wait()
        row = lax.broadcasted_iota(jnp.int32, (cells, products * stores), 0)
        col = lax.broadcasted_iota(jnp.int32, (cells, products * stores), 1)
        store = mod(lax.broadcasted_iota(jnp.int32, (1, products * stores), 1), stores)
        region = jnp.zeros((1, products * stores), jnp.int32)
        for s in range(stores):
            region = jnp.where(store == s, sr[s], region)
        hot = jnp.where(
            (div(row, REGION_COUNT) == div(col, stores)) & (mod(row, REGION_COUNT) == region), 1.0, 0.0
        ).astype(jnp.bfloat16)
        acc[...] = jnp.zeros_like(acc)
        for i in range(CHUNKS):
            loads[i].wait()
            side = 0 if 2 * i < CHUNKS else 2
            flags = [
                jnp.where(dm[t * days + i * step + d] == t, 1.0, 0.0).astype(jnp.float32) for d in range(step)
            ]
            for p in range(products):
                outer, inner = acc[side, p], acc[1, p]
                for d in range(step):
                    x = buf[i * step + d, p]
                    inner = inner + x * flags[d]
                    outer = outer + x * (1.0 - flags[d])
                acc[side, p], acc[1, p] = outer, inner
        sums = select_rows(hot, [acc[k].reshape(products * stores, measures) for k in range(3)])
        years = [my[jnp.clip(t - 1 + k, 0, months - 1)] for k in range(3)]
        for j in range(half):
            for ref, year in ((keep, b * half + j), (send, (1 - b) * half + j)):
                total = jnp.where(years[0] == year, sums[0], 0.0)
                total = total + jnp.where(years[1] == year, sums[1], 0.0)
                total = total + jnp.where(years[2] == year, sums[2], 0.0)
                ref[pl.ds(j * cells, cells)] = total
        send[pl.ds(half * cells, cells)] = jnp.where(b == 0, sums[2], sums[0])
        far[...] = jnp.where(b == 0, sums[0], sums[2])
        own[...] = sums[1]

    f32 = jnp.float32
    return pl.pallas_call(
        kernel,
        out_shape=[
            jax.ShapeDtypeStruct((half * cells, measures), f32),
            jax.ShapeDtypeStruct((half * cells + cells, measures), f32),
            jax.ShapeDtypeStruct((cells, measures), f32),
            jax.ShapeDtypeStruct((cells, measures), f32),
        ],
        in_specs=[ANY] * 4,
        out_specs=[VMEM] * 4,
        scratch_shapes=[
            pltpu.VMEM(sales.shape, f32),
            pltpu.SMEM(day_month.shape, jnp.int32),
            pltpu.SMEM(month_year.shape, jnp.int32),
            pltpu.SMEM(store_region.shape, jnp.int32),
            pltpu.VMEM((3, products, stores, measures), f32),
            pltpu.SemaphoreType.DMA((CHUNKS,)),
            pltpu.SemaphoreType.DMA((3,)),
        ],
        name="local_sums",
    )(sales, day_month, month_year, store_region)


def roll_up_rows(cats):
    return -(-(cats * REGION_COUNT + cats + REGION_COUNT + 1) // 8) * 8


def tables(day_month, month_year, product_category, store_region, year_count, cats, first, with_month):
    products, stores = product_category.shape[0], store_region.shape[0]
    months = month_year.shape[0]
    rows, cells = roll_up_rows(cats), products * REGION_COUNT
    a, c0, r0 = cats * REGION_COUNT, cats * REGION_COUNT + cats, cats * REGION_COUNT + cats + REGION_COUNT

    def kernel(dm, my, pc, sr, hot, factor):
        t = lax.axis_index("tm")
        base = first()

        def row_keys(shape):
            i = lax.broadcasted_iota(jnp.int32, shape, 0)
            cat = jnp.where(i < a, div(i, REGION_COUNT), jnp.where(i < c0, i - a, -1))
            reg = jnp.where(i < a, mod(i, REGION_COUNT), jnp.where((i >= c0) & (i < r0), i - c0, -1))
            return i, jnp.where(cat >= 0, cat + base, -1), reg

        i, cat, reg = row_keys((rows, cells))
        col = lax.broadcasted_iota(jnp.int32, (1, cells), 1)
        label = jnp.zeros((1, cells), jnp.int32)
        for p in range(products):
            label = jnp.where(div(col, REGION_COUNT) == p, pc[p], label)
        hit = ((cat < 0) | (cat == label)) & ((reg < 0) | (reg == mod(col, REGION_COUNT))) & (i <= r0)
        hot[...] = jnp.where(hit, 1.0, 0.0).astype(jnp.bfloat16)

        lanes = 128
        i, cat, reg = row_keys((rows, lanes))
        size = jnp.where(cat < 0, float(products), 0.0)
        for p in range(products):
            size = size + jnp.where(cat == pc[p], 1.0, 0.0)
        area = jnp.where(reg < 0, float(stores), 0.0)
        for s in range(stores):
            area = area + jnp.where(reg == sr[s], 1.0, 0.0)
        lane = lax.broadcasted_iota(jnp.int32, (1, lanes), 1)
        days = jnp.ones((1, lanes), jnp.float32)
        day = dm[...]

        def count(low, high):
            return jnp.sum(jnp.where((day >= low) & (day < high), 1.0, 0.0))

        bounds = [jnp.int32(0)] * (year_count + 1)
        for m in range(months):
            year = my[m]
            for y in range(1, year_count):
                bounds[y] = bounds[y] + jnp.where(year < y, 1, 0)
        bounds[year_count] = jnp.int32(months)
        for y in range(year_count):
            days = jnp.where(lane == y, count(bounds[y], bounds[y + 1]), days)
        days = jnp.where(lane == year_count, count(t, t + 1), days)
        cell = days * size * area
        factor[...] = 1.0 / jnp.sqrt(jnp.where(i == r0, cell, jnp.maximum(cell, 1.0)))

    return pl.pallas_call(
        kernel,
        out_shape=[
            jax.ShapeDtypeStruct((rows, cells), jnp.bfloat16),
            jax.ShapeDtypeStruct((rows, 128), jnp.float32),
        ],
        in_specs=[VMEM, SMEM, SMEM, SMEM],
        out_specs=[VMEM] * 2,
        name="tables",
    )(day_month.reshape(-1, 128), month_year, product_category, store_region)


def roll_up(hot, factor, lower, upper, months, year_count, cats):
    cells = hot.shape[1]
    measures = (lower if lower is not None else months[0]).shape[1]
    half = year_count // 2
    a, c0, r0 = cats * REGION_COUNT, cats * REGION_COUNT + cats, cats * REGION_COUNT + cats + REGION_COUNT
    years = [lower, upper]
    groups = year_count + 1

    def kernel(hot, factor, lower, upper, own, near, far, *outs):
        even = lax.rem(lax.axis_index("tm"), 2) == 0
        blocks = []
        for h in range(2):
            for j in range(half):
                x, y = lower[pl.ds(j * cells, cells)], upper[pl.ds(j * cells, cells)]
                blocks.append(jnp.where(even, x, y) if h == 0 else jnp.where(even, y, x))
        blocks.append(own[...] + near[...] + far[...])
        done = select_rows(hot[...], blocks)
        for g in range(groups):
            x = done[g] * factor[:, g : g + 1]
            refs = outs[4:] if g < year_count else outs[:4]
            at = g if g < year_count else 0
            refs[0][at] = x[:a]
            refs[1][at] = x[a:c0]
            refs[2][at] = x[c0:r0]
            refs[3][pl.ds(at, 1)] = x[r0 : r0 + 1]

    def shapes(n):
        return [
            jax.ShapeDtypeStruct((n, a, measures), jnp.float32),
            jax.ShapeDtypeStruct((n, cats, measures), jnp.float32),
            jax.ShapeDtypeStruct((n, REGION_COUNT, measures), jnp.float32),
            jax.ShapeDtypeStruct((n, measures), jnp.float32),
        ]

    outs = list(pl.pallas_call(
        kernel,
        out_shape=shapes(1) + shapes(year_count),
        in_specs=[VMEM] * 7,
        out_specs=[VMEM] * 8,
        name="roll_up",
    )(hot, factor, lower, upper, *months))
    for k, n in ((0, 1), (4, year_count)):
        outs[k] = outs[k].reshape(n, cats, REGION_COUNT, measures)
    return outs


def shards(sales_records, day_month, month_year, product_category, store_region):
    count = lax.axis_size("tm")
    year_count = max(month_year.shape[0] // 8, 2)
    cells = sales_records.shape[1] * REGION_COUNT
    half = year_count // 2 * cells

    def swap(x, distance):
        return lax.ppermute(x, "tm", [(i, i ^ distance) for i in range(count)])

    keep, send, own, far = local_sums(sales_records, day_month, month_year, store_region, year_count)
    got = swap(send, 1)
    years, near = keep + got[:half], got[half:]
    distances = [1 << k for k in range(1, log2(count))]
    if len(distances) > 1:
        distances[-2:] = distances[:-3:-1]
    edge = {0: 0, count - 1: count - 1}
    across = [(i, edge.get(i, i + 1 if i % 2 else i - 1)) for i in range(count)]
    for k, d in enumerate(distances):
        if k == len(distances) - 1:
            far, years = lax.optimization_barrier((far, years))
        years = years + swap(years, d)
        if k == len(distances) - 1:
            far = lax.ppermute(far, "tm", across)
    other = swap(years, 1)
    prods = lax.axis_size("prod")
    cats = CATEGORY_COUNT // prods
    if prods == 1:
        hot, factor = tables(
            day_month, month_year, product_category, store_region, year_count, cats, lambda: 0, True
        )
        return tuple(roll_up(hot, factor, years, other, (own, near, far), year_count, cats))

    def gathered(x):
        x = lax.all_gather(x.reshape(-1, cells, x.shape[-1]), "prod", axis=1, tiled=True)
        return x.reshape(-1, x.shape[-1])

    years, other, own, near, far = [gathered(x) for x in (years, other, own, near, far)]
    outs = []
    for n, first in ((cats, lambda: lax.axis_index("prod") * cats), (CATEGORY_COUNT, lambda: 0)):
        hot, factor = tables(day_month, month_year, product_category, store_region, year_count, n, first, True)
        outs.append(roll_up(hot, factor, years, other, (own, near, far), year_count, n))
    return tuple(outs[0][:4]) + tuple(outs[1][4:])


def solution(mesh):
    placed = (P("tm", "prod", None, None), P(), P(), P(), P())
    return jax.shard_map(
        shards,
        mesh=mesh,
        in_specs=placed,
        out_specs=(
            P("tm", "prod", None, None),
            P("tm", "prod", None),
            P("tm", None, None),
            P("tm", None),
            P(),
            P(),
            P(),
            P(),
        ),
        check_vma=False,
    )
```

```python
import jax
import jax.numpy as jnp
from jax import lax
from jax.experimental import pallas as pl
from jax.experimental.pallas import tpu as pltpu
from jax.sharding import PartitionSpec as P

CATEGORY_COUNT = 32
REGION_COUNT = 4
CHUNKS = 8
VMEM = pl.BlockSpec(memory_space=pltpu.VMEM)
SMEM = pl.BlockSpec(memory_space=pltpu.SMEM)
ANY = pl.BlockSpec(memory_space=pl.ANY)


def log2(n):
    assert n & (n - 1) == 0
    return n.bit_length() - 1


def div(x, n):
    return lax.shift_right_logical(x, jnp.int32(log2(n)))


def mod(x, n):
    return lax.bitwise_and(x, jnp.int32(n - 1))


def pieces(x):
    high = x.astype(jnp.bfloat16)
    rest = x - high.astype(jnp.float32)
    mid = rest.astype(jnp.bfloat16)
    low = (rest - mid.astype(jnp.float32)).astype(jnp.bfloat16)
    return [high, mid, low]


def select_rows(hot, blocks):
    width = blocks[0].shape[1]
    out = jnp.dot(
        hot, jnp.concatenate([t for b in blocks for t in pieces(b)], axis=1), preferred_element_type=jnp.float32
    )
    cut = [out[:, i * width : (i + 1) * width] for i in range(3 * len(blocks))]
    return [(cut[3 * i + 2] + cut[3 * i + 1]) + cut[3 * i] for i in range(len(blocks))]


def local_sums(sales, day_month, month_year, store_region, year_count):
    days, products, stores, measures = sales.shape
    cells = products * REGION_COUNT
    half = year_count // 2
    step = days // CHUNKS
    months = month_year.shape[0]

    def kernel(sales_hbm, dm_hbm, my_hbm, sr_hbm, keep, send, own, far, buf, dm, my, sr, acc, sems, small):
        t = lax.axis_index("tm")
        b = lax.rem(t, 2)
        copies = [
            pltpu.make_async_copy(s, d, small.at[i])
            for i, (s, d) in enumerate(((dm_hbm, dm), (my_hbm, my), (sr_hbm, sr)))
        ]
        for c in copies:
            c.start()
        loads = [
            pltpu.make_async_copy(sales_hbm.at[pl.ds(i * step, step)], buf.at[pl.ds(i * step, step)], sems.at[i])
            for i in range(CHUNKS)
        ]
        for c in loads:
            c.start()
        for c in copies:
            c.wait()
        row = lax.broadcasted_iota(jnp.int32, (cells, products * stores), 0)
        col = lax.broadcasted_iota(jnp.int32, (cells, products * stores), 1)
        store = mod(lax.broadcasted_iota(jnp.int32, (1, products * stores), 1), stores)
        region = jnp.zeros((1, products * stores), jnp.int32)
        for s in range(stores):
            region = jnp.where(store == s, sr[s], region)
        hot = jnp.where(
            (div(row, REGION_COUNT) == div(col, stores)) & (mod(row, REGION_COUNT) == region), 1.0, 0.0
        ).astype(jnp.bfloat16)
        acc[...] = jnp.zeros_like(acc)
        for i in range(CHUNKS):
            loads[i].wait()
            side = 0 if 2 * i < CHUNKS else 2
            flags = [
                jnp.where(dm[t * days + i * step + d] == t, 1.0, 0.0).astype(jnp.float32) for d in range(step)
            ]
            for p in range(products):
                outer, inner = acc[side, p], acc[1, p]
                for d in range(step):
                    x = buf[i * step + d, p]
                    inner = inner + x * flags[d]
                    outer = outer + x * (1.0 - flags[d])
                acc[side, p], acc[1, p] = outer, inner
        sums = select_rows(hot, [acc[k].reshape(products * stores, measures) for k in range(3)])
        years = [my[jnp.clip(t - 1 + k, 0, months - 1)] for k in range(3)]
        for j in range(half):
            for ref, year in ((keep, b * half + j), (send, (1 - b) * half + j)):
                total = jnp.where(years[0] == year, sums[0], 0.0)
                total = total + jnp.where(years[1] == year, sums[1], 0.0)
                total = total + jnp.where(years[2] == year, sums[2], 0.0)
                ref[pl.ds(j * cells, cells)] = total
        send[pl.ds(half * cells, cells)] = jnp.where(b == 0, sums[2], sums[0])
        far[...] = jnp.where(b == 0, sums[0], sums[2])
        own[...] = sums[1]

    f32 = jnp.float32
    return pl.pallas_call(
        kernel,
        out_shape=[
            pltpu.VMEM((half * cells, measures), f32),
            pltpu.VMEM((half * cells + cells, measures), f32),
            pltpu.VMEM((cells, measures), f32),
            pltpu.VMEM((cells, measures), f32),
        ],
        in_specs=[ANY] * 4,
        out_specs=[VMEM] * 4,
        scratch_shapes=[
            pltpu.VMEM(sales.shape, f32),
            pltpu.SMEM(day_month.shape, jnp.int32),
            pltpu.SMEM(month_year.shape, jnp.int32),
            pltpu.SMEM(store_region.shape, jnp.int32),
            pltpu.VMEM((3, products, stores, measures), f32),
            pltpu.SemaphoreType.DMA((CHUNKS,)),
            pltpu.SemaphoreType.DMA((3,)),
        ],
        name="local_sums",
    )(sales, day_month, month_year, store_region)


def roll_up_rows(cats):
    return -(-(cats * REGION_COUNT + cats + REGION_COUNT + 1) // 8) * 8


def tables(day_month, month_year, product_category, store_region, year_count, cats, first):
    products, stores = product_category.shape[0], store_region.shape[0]
    months = month_year.shape[0]
    rows, cells = roll_up_rows(cats), products * REGION_COUNT
    a, c0, r0 = cats * REGION_COUNT, cats * REGION_COUNT + cats, cats * REGION_COUNT + cats + REGION_COUNT

    def kernel(dm, my, pc, sr, hot, factor):
        t = lax.axis_index("tm")
        base = first()

        def row_keys(shape):
            i = lax.broadcasted_iota(jnp.int32, shape, 0)
            cat = jnp.where(i < a, div(i, REGION_COUNT), jnp.where(i < c0, i - a, -1))
            reg = jnp.where(i < a, mod(i, REGION_COUNT), jnp.where((i >= c0) & (i < r0), i - c0, -1))
            return i, jnp.where(cat >= 0, cat + base, -1), reg

        i, cat, reg = row_keys((rows, cells))
        col = lax.broadcasted_iota(jnp.int32, (1, cells), 1)
        label = jnp.zeros((1, cells), jnp.int32)
        for p in range(products):
            label = jnp.where(div(col, REGION_COUNT) == p, pc[p], label)
        hit = ((cat < 0) | (cat == label)) & ((reg < 0) | (reg == mod(col, REGION_COUNT))) & (i <= r0)
        hot[...] = jnp.where(hit, 1.0, 0.0).astype(jnp.bfloat16)

        lanes = 128
        i, cat, reg = row_keys((rows, lanes))
        size = jnp.where(cat < 0, float(products), 0.0)
        for p in range(products):
            size = size + jnp.where(cat == pc[p], 1.0, 0.0)
        area = jnp.where(reg < 0, float(stores), 0.0)
        for s in range(stores):
            area = area + jnp.where(reg == sr[s], 1.0, 0.0)
        lane = lax.broadcasted_iota(jnp.int32, (1, lanes), 1)
        days = jnp.ones((1, lanes), jnp.float32)
        day = dm[...]

        def count(low, high):
            return jnp.sum(jnp.where((day >= low) & (day < high), 1.0, 0.0))

        bounds = [jnp.int32(0)] * (year_count + 1)
        for m in range(months):
            year = my[m]
            for y in range(1, year_count):
                bounds[y] = bounds[y] + jnp.where(year < y, 1, 0)
        bounds[year_count] = jnp.int32(months)
        for y in range(year_count):
            days = jnp.where(lane == y, count(bounds[y], bounds[y + 1]), days)
        days = jnp.where(lane == year_count, count(t, t + 1), days)
        cell = days * size * area
        factor[...] = 1.0 / jnp.sqrt(jnp.where(i == r0, cell, jnp.maximum(cell, 1.0)))

    return pl.pallas_call(
        kernel,
        out_shape=[
            pltpu.VMEM((rows, cells), jnp.bfloat16),
            pltpu.VMEM((rows, 128), jnp.float32),
        ],
        in_specs=[VMEM, SMEM, SMEM, SMEM],
        out_specs=[VMEM] * 2,
        name="tables",
    )(day_month.reshape(-1, 128), month_year, product_category, store_region)


def roll_up(hot, factor, lower, upper, months, year_count, cats):
    cells = hot.shape[1]
    measures = (lower if lower is not None else months[0]).shape[1]
    half = year_count // 2
    a, c0, r0 = cats * REGION_COUNT, cats * REGION_COUNT + cats, cats * REGION_COUNT + cats + REGION_COUNT
    groups = year_count + 1

    def kernel(hot, factor, lower, upper, own, near, far, *outs):
        even = lax.rem(lax.axis_index("tm"), 2) == 0
        blocks = []
        for h in range(2):
            for j in range(half):
                x, y = lower[pl.ds(j * cells, cells)], upper[pl.ds(j * cells, cells)]
                blocks.append(jnp.where(even, x, y) if h == 0 else jnp.where(even, y, x))
        blocks.append(own[...] + near[...] + far[...])
        done = select_rows(hot[...], blocks)
        for g in range(groups):
            x = done[g] * factor[:, g : g + 1]
            refs = outs[4:] if g < year_count else outs[:4]
            at = g if g < year_count else 0
            refs[0][at] = x[:a]
            refs[1][at] = x[a:c0]
            refs[2][at] = x[c0:r0]
            refs[3][pl.ds(at, 1)] = x[r0 : r0 + 1]

    def shapes(n):
        return [
            jax.ShapeDtypeStruct((n, a, measures), jnp.float32),
            jax.ShapeDtypeStruct((n, cats, measures), jnp.float32),
            jax.ShapeDtypeStruct((n, REGION_COUNT, measures), jnp.float32),
            jax.ShapeDtypeStruct((n, measures), jnp.float32),
        ]

    outs = list(pl.pallas_call(
        kernel,
        out_shape=shapes(1) + shapes(year_count),
        in_specs=[VMEM] * 7,
        out_specs=[VMEM] * 8,
        name="roll_up",
    )(*[pltpu.with_memory_space_constraint(x, pltpu.VMEM) for x in (hot, factor, lower, upper, *months)]))
    for k, n in ((0, 1), (4, year_count)):
        outs[k] = outs[k].reshape(n, cats, REGION_COUNT, measures)
    return outs


def cube(sales_records, day_month, month_year, product_category, store_region):
    count = lax.axis_size("tm")
    year_count = max(month_year.shape[0] // 8, 2)
    cells = sales_records.shape[1] * REGION_COUNT
    half = year_count // 2 * cells

    def swap(x, distance):
        return lax.ppermute(x, "tm", [(i, i ^ distance) for i in range(count)])

    keep, send, own, far = local_sums(sales_records, day_month, month_year, store_region, year_count)
    got = swap(send, 1)
    years, near = keep + got[:half], got[half:]
    distances = [1 << k for k in range(1, log2(count))]
    if len(distances) > 1:
        distances[-2:] = distances[:-3:-1]
    edge = {0: 0, count - 1: count - 1}
    across = [(i, edge.get(i, i + 1 if i % 2 else i - 1)) for i in range(count)]
    prods = lax.axis_size("prod")
    cats = CATEGORY_COUNT // prods
    if prods == 1:
        hot, factor = tables(day_month, month_year, product_category, store_region, year_count, cats, lambda: 0)
    busiest = len(distances) - 2
    for k, d in enumerate(distances):
        if k == 1 and prods == 1:
            years, hot, factor = lax.optimization_barrier((years, hot, factor))
        if k == busiest:
            far, years = lax.optimization_barrier((far, years))
            far = lax.ppermute(far, "tm", across)
        years = years + swap(years, d)
    other = swap(years, 1)
    if prods == 1:
        return tuple(roll_up(hot, factor, years, other, (own, near, far), year_count, cats))

    def gathered(x):
        x = lax.all_gather(x.reshape(-1, cells, x.shape[-1]), "prod", axis=1, tiled=True)
        return x.reshape(-1, x.shape[-1])

    years, other, own, near, far = [gathered(x) for x in (years, other, own, near, far)]
    outs = []
    for n, first in ((cats, lambda: lax.axis_index("prod") * cats), (CATEGORY_COUNT, lambda: 0)):
        hot, factor = tables(day_month, month_year, product_category, store_region, year_count, n, first)
        outs.append(roll_up(hot, factor, years, other, (own, near, far), year_count, n))
    return tuple(outs[0][:4]) + tuple(outs[1][4:])


def solution(mesh):
    placed = (P("tm", "prod", None, None), P(), P(), P(), P())
    return jax.shard_map(
        cube,
        mesh=mesh,
        in_specs=placed,
        out_specs=(
            P("tm", "prod", None, None),
            P("tm", "prod", None),
            P("tm", None, None),
            P("tm", None),
            P(),
            P(),
            P(),
            P(),
        ),
        check_vma=False,
    )
```

```python
import jax
import jax.numpy as jnp
from jax import lax
from jax.experimental import pallas as pl
from jax.experimental.pallas import tpu as pltpu
from jax.sharding import PartitionSpec as P

CATEGORY_COUNT = 32
REGION_COUNT = 4
CHUNKS = 8
VMEM = pl.BlockSpec(memory_space=pltpu.VMEM)
SMEM = pl.BlockSpec(memory_space=pltpu.SMEM)
ANY = pl.BlockSpec(memory_space=pl.ANY)


def rounds_of(count):
    bits = [1 << k for k in range(1, log2(count))]
    rounds = []
    while bits:
        pair = bits[:: max(len(bits) // 2, 1)][:2]
        bits = [b for b in bits if b not in pair]
        rounds.append(tuple((pair[0] + pair[1], pair[1], pair[0])) if len(pair) > 1 else tuple(pair))
    return rounds


def log2(n):
    assert n & (n - 1) == 0
    return n.bit_length() - 1


def div(x, n):
    return lax.shift_right_logical(x, jnp.int32(log2(n)))


def mod(x, n):
    return lax.bitwise_and(x, jnp.int32(n - 1))


def pieces(x):
    high = x.astype(jnp.bfloat16)
    rest = x - high.astype(jnp.float32)
    mid = rest.astype(jnp.bfloat16)
    low = (rest - mid.astype(jnp.float32)).astype(jnp.bfloat16)
    return [high, mid, low]


def select_rows(hot, blocks):
    width = blocks[0].shape[1]
    out = jnp.dot(
        hot, jnp.concatenate([t for b in blocks for t in pieces(b)], axis=1), preferred_element_type=jnp.float32
    )
    cut = [out[:, i * width : (i + 1) * width] for i in range(3 * len(blocks))]
    return [(cut[3 * i + 2] + cut[3 * i + 1]) + cut[3 * i] for i in range(len(blocks))]


def local_sums(sales, day_month, month_year, store_region, year_count):
    days, products, stores, measures = sales.shape
    cells = products * REGION_COUNT
    half = year_count // 2
    step = days // CHUNKS
    months = month_year.shape[0]

    def kernel(sales_hbm, dm_hbm, my_hbm, sr_hbm, keep, send, own, far, buf, dm, my, sr, acc, sems, small):
        t = lax.axis_index("tm")
        b = lax.rem(t, 2)
        copies = [
            pltpu.make_async_copy(s, d, small.at[i])
            for i, (s, d) in enumerate(((dm_hbm, dm), (my_hbm, my), (sr_hbm, sr)))
        ]
        for c in copies:
            c.start()
        loads = [
            pltpu.make_async_copy(sales_hbm.at[pl.ds(i * step, step)], buf.at[pl.ds(i * step, step)], sems.at[i])
            for i in range(CHUNKS)
        ]
        for c in loads:
            c.start()
        for c in copies:
            c.wait()
        row = lax.broadcasted_iota(jnp.int32, (cells, products * stores), 0)
        col = lax.broadcasted_iota(jnp.int32, (cells, products * stores), 1)
        store = mod(lax.broadcasted_iota(jnp.int32, (1, products * stores), 1), stores)
        region = jnp.zeros((1, products * stores), jnp.int32)
        for s in range(stores):
            region = jnp.where(store == s, sr[s], region)
        hot = jnp.where(
            (div(row, REGION_COUNT) == div(col, stores)) & (mod(row, REGION_COUNT) == region), 1.0, 0.0
        ).astype(jnp.bfloat16)
        acc[...] = jnp.zeros_like(acc)
        for i in range(CHUNKS):
            loads[i].wait()
            side = 0 if 2 * i < CHUNKS else 2
            flags = [
                jnp.where(dm[t * days + i * step + d] == t, 1.0, 0.0).astype(jnp.float32) for d in range(step)
            ]
            for p in range(products):
                outer, inner = acc[side, p], acc[1, p]
                for d in range(step):
                    x = buf[i * step + d, p]
                    inner = inner + x * flags[d]
                    outer = outer + x * (1.0 - flags[d])
                acc[side, p], acc[1, p] = outer, inner
        sums = select_rows(hot, [acc[k].reshape(products * stores, measures) for k in range(3)])
        years = [my[jnp.clip(t - 1 + k, 0, months - 1)] for k in range(3)]
        for j in range(half):
            for ref, year in ((keep, b * half + j), (send, (1 - b) * half + j)):
                total = jnp.where(years[0] == year, sums[0], 0.0)
                total = total + jnp.where(years[1] == year, sums[1], 0.0)
                total = total + jnp.where(years[2] == year, sums[2], 0.0)
                ref[pl.ds(j * cells, cells)] = total
        send[pl.ds(half * cells, cells)] = jnp.where(b == 0, sums[2], sums[0])
        far[...] = jnp.where(b == 0, sums[0], sums[2])
        own[...] = sums[1]

    f32 = jnp.float32
    return pl.pallas_call(
        kernel,
        out_shape=[
            pltpu.VMEM((half * cells, measures), f32),
            pltpu.VMEM((half * cells + cells, measures), f32),
            pltpu.VMEM((cells, measures), f32),
            pltpu.VMEM((cells, measures), f32),
        ],
        in_specs=[ANY] * 4,
        out_specs=[VMEM] * 4,
        scratch_shapes=[
            pltpu.VMEM(sales.shape, f32),
            pltpu.SMEM(day_month.shape, jnp.int32),
            pltpu.SMEM(month_year.shape, jnp.int32),
            pltpu.SMEM(store_region.shape, jnp.int32),
            pltpu.VMEM((3, products, stores, measures), f32),
            pltpu.SemaphoreType.DMA((CHUNKS,)),
            pltpu.SemaphoreType.DMA((3,)),
        ],
        name="local_sums",
    )(sales, day_month, month_year, store_region)


def roll_up_rows(cats):
    return -(-(cats * REGION_COUNT + cats + REGION_COUNT + 1) // 8) * 8


def tables(day_month, month_year, product_category, store_region, year_count, cats, first):
    products, stores = product_category.shape[0], store_region.shape[0]
    months = month_year.shape[0]
    rows, cells = roll_up_rows(cats), products * REGION_COUNT
    a, c0, r0 = cats * REGION_COUNT, cats * REGION_COUNT + cats, cats * REGION_COUNT + cats + REGION_COUNT

    def kernel(dm, my, pc, sr, hot, factor):
        t = lax.axis_index("tm")
        base = first()

        def row_keys(shape):
            i = lax.broadcasted_iota(jnp.int32, shape, 0)
            cat = jnp.where(i < a, div(i, REGION_COUNT), jnp.where(i < c0, i - a, -1))
            reg = jnp.where(i < a, mod(i, REGION_COUNT), jnp.where((i >= c0) & (i < r0), i - c0, -1))
            return i, jnp.where(cat >= 0, cat + base, -1), reg

        i, cat, reg = row_keys((rows, cells))
        col = lax.broadcasted_iota(jnp.int32, (1, cells), 1)
        label = jnp.zeros((1, cells), jnp.int32)
        for p in range(products):
            label = jnp.where(div(col, REGION_COUNT) == p, pc[p], label)
        hit = ((cat < 0) | (cat == label)) & ((reg < 0) | (reg == mod(col, REGION_COUNT))) & (i <= r0)
        hot[...] = jnp.where(hit, 1.0, 0.0).astype(jnp.bfloat16)

        lanes = 128
        i, cat, reg = row_keys((rows, lanes))
        size = jnp.where(cat < 0, float(products), 0.0)
        for p in range(products):
            size = size + jnp.where(cat == pc[p], 1.0, 0.0)
        area = jnp.where(reg < 0, float(stores), 0.0)
        for s in range(stores):
            area = area + jnp.where(reg == sr[s], 1.0, 0.0)
        lane = lax.broadcasted_iota(jnp.int32, (1, lanes), 1)
        days = jnp.ones((1, lanes), jnp.float32)
        day = dm[...]

        def count(low, high):
            return jnp.sum(jnp.where((day >= low) & (day < high), 1.0, 0.0))

        bounds = [jnp.int32(0)] * (year_count + 1)
        for m in range(months):
            year = my[m]
            for y in range(1, year_count):
                bounds[y] = bounds[y] + jnp.where(year < y, 1, 0)
        bounds[year_count] = jnp.int32(months)
        for y in range(year_count):
            days = jnp.where(lane == y, count(bounds[y], bounds[y + 1]), days)
        days = jnp.where(lane == year_count, count(t, t + 1), days)
        cell = days * size * area
        factor[...] = 1.0 / jnp.sqrt(jnp.where(i == r0, cell, jnp.maximum(cell, 1.0)))

    return pl.pallas_call(
        kernel,
        out_shape=[
            pltpu.VMEM((rows, cells), jnp.bfloat16),
            pltpu.VMEM((rows, 128), jnp.float32),
        ],
        in_specs=[VMEM, SMEM, SMEM, SMEM],
        out_specs=[VMEM] * 2,
        name="tables",
    )(day_month.reshape(-1, 128), month_year, product_category, store_region)


def roll_up(hot, factor, lower, upper, months, year_count, cats):
    cells = hot.shape[1]
    measures = (lower if lower is not None else months[0]).shape[1]
    half = year_count // 2
    a, c0, r0 = cats * REGION_COUNT, cats * REGION_COUNT + cats, cats * REGION_COUNT + cats + REGION_COUNT
    groups = year_count + 1

    def kernel(hot, factor, lower, upper, own, near, far, *outs):
        even = lax.rem(lax.axis_index("tm"), 2) == 0
        blocks = []
        for h in range(2):
            for j in range(half):
                x, y = lower[pl.ds(j * cells, cells)], upper[pl.ds(j * cells, cells)]
                blocks.append(jnp.where(even, x, y) if h == 0 else jnp.where(even, y, x))
        blocks.append(own[...] + near[...] + far[...])
        done = select_rows(hot[...], blocks)
        for g in range(groups):
            x = done[g] * factor[:, g : g + 1]
            refs = outs[4:] if g < year_count else outs[:4]
            at = g if g < year_count else 0
            refs[0][at] = x[:a]
            refs[1][at] = x[a:c0]
            refs[2][at] = x[c0:r0]
            refs[3][pl.ds(at, 1)] = x[r0 : r0 + 1]

    def shapes(n):
        return [
            jax.ShapeDtypeStruct((n, a, measures), jnp.float32),
            jax.ShapeDtypeStruct((n, cats, measures), jnp.float32),
            jax.ShapeDtypeStruct((n, REGION_COUNT, measures), jnp.float32),
            jax.ShapeDtypeStruct((n, measures), jnp.float32),
        ]

    outs = list(pl.pallas_call(
        kernel,
        out_shape=shapes(1) + shapes(year_count),
        in_specs=[VMEM] * 7,
        out_specs=[VMEM] * 8,
        name="roll_up",
    )(*[pltpu.with_memory_space_constraint(x, pltpu.VMEM) for x in (hot, factor, lower, upper, *months)]))
    for k, n in ((0, 1), (4, year_count)):
        outs[k] = outs[k].reshape(n, cats, REGION_COUNT, measures)
    return outs


def cube(sales_records, day_month, month_year, product_category, store_region):
    count = lax.axis_size("tm")
    year_count = max(month_year.shape[0] // 8, 2)
    cells = sales_records.shape[1] * REGION_COUNT
    half = year_count // 2 * cells

    def swap(x, distance):
        return lax.ppermute(x, "tm", [(i, i ^ distance) for i in range(count)])

    keep, send, own, far = local_sums(sales_records, day_month, month_year, store_region, year_count)
    got = swap(send, 1)
    years, near = keep + got[:half], got[half:]
    rounds = rounds_of(count)
    edge = {0: 0, count - 1: count - 1}
    across = [(i, edge.get(i, i + 1 if i % 2 else i - 1)) for i in range(count)]
    prods = lax.axis_size("prod")
    cats = CATEGORY_COUNT // prods
    if prods == 1:
        hot, factor = tables(day_month, month_year, product_category, store_region, year_count, cats, lambda: 0)
    for k, distances in enumerate(rounds):
        if k == 1 and prods == 1:
            years, hot, factor = lax.optimization_barrier((years, hot, factor))
        if k == len(rounds) - 1:
            far, years = lax.optimization_barrier((far, years))
            far = lax.ppermute(far, "tm", across)
        total = years
        for d in distances:
            total = total + swap(years, d)
        years = total
    other = swap(years, 1)
    if prods == 1:
        return tuple(roll_up(hot, factor, years, other, (own, near, far), year_count, cats))

    def gathered(x):
        x = lax.all_gather(x.reshape(-1, cells, x.shape[-1]), "prod", axis=1, tiled=True)
        return x.reshape(-1, x.shape[-1])

    years, other, own, near, far = [gathered(x) for x in (years, other, own, near, far)]
    outs = []
    for n, first in ((cats, lambda: lax.axis_index("prod") * cats), (CATEGORY_COUNT, lambda: 0)):
        hot, factor = tables(day_month, month_year, product_category, store_region, year_count, n, first)
        outs.append(roll_up(hot, factor, years, other, (own, near, far), year_count, n))
    return tuple(outs[0][:4]) + tuple(outs[1][4:])


def solution(mesh):
    placed = (P("tm", "prod", None, None), P(), P(), P(), P())
    return jax.shard_map(
        cube,
        mesh=mesh,
        in_specs=placed,
        out_specs=(
            P("tm", "prod", None, None),
            P("tm", "prod", None),
            P("tm", None, None),
            P("tm", None),
            P(),
            P(),
            P(),
            P(),
        ),
        check_vma=False,
    )
```
